32 devices in a mesh: grp: 2 (over x), ep: 16 (over z, y, core).
Axes of the slice: x: 2, y: 2, z: 4, core: 2. Of those that a mesh axis runs over, the one named last changes fastest.
Arguments:
- expert_ids: int32 [2048, 8], P(('grp', 'ep')), parts along dimension 0, may hold values from 0 to 15, all different within a row; in each aligned block of 64 rows (0 to 63, 64 to 127, ...) at most 64 rows name the same one
- route_gates: float32 [2048, 8], P(('grp', 'ep')), parts along dimension 0, may hold values from 0.1 to 0.5
- routed_in: bfloat16 [2048, 8, 2048], P(('grp', 'ep')), parts along dimension 0, may hold values from -6 to 6
- down_weight: bfloat16 [16, 1024, 3584], P('ep'), may hold values from -0.1875 to 0.1875
- slot_offset: int32 [1], replicated, may hold values from 0 to 15
Outputs:
- combined: bfloat16 [2048, 3584], P(('grp', 'ep')), parts along dimension 0
The draws below stay inside these ranges and needn't reach their ends.
There are 2 independent parts, one for each index of `grp`. The reference program is written for one: setup_inputs(seed, part) draws one part's arguments, and reference() takes and returns one part's arrays. A program takes and returns all parts, laid end to end along the dimension named above; an argument that names none is the same for every part. Nothing has to cross between parts.
Inputs may be any that keep to these rules, and one draw needn't show every extreme that they name: `expert_ids`: each row names 8 different experts. Among the tokens of one ep device, no expert is named by more than 64 tokens, a bound that some block reaches in some devices.
All inputs are finite; a program needn't handle non-finite values.
Results may differ from the reference program's by a relative error of at most 0.0057.
Values may be sent and summed in bfloat16 or wider, within the bound.
A program may use at most 128 MiB of HBM per device.

```python
import math
import jax
import jax.numpy as jnp
import numpy as np
from jax import lax

D = 3584
F = 1024
TOP = 8
TOK_DEV = 64
EXPERTS = 16
TOKENS = 1024
CAP = 64


def levels(stream_key, extent, split, smallest, largest):
    loudness = 1.0
    for dim, blocks in split:
        heights = jax.random.uniform(jax.random.fold_in(jax.random.fold_in(stream_key, 6), dim), (blocks,), jnp.float32, smallest / len(split), largest / len(split))
        loudness = loudness * jnp.repeat(jnp.exp(heights), extent[dim] // blocks).reshape((-1,) + (1,) * (len(extent) - 1 - dim))
    return loudness


def routed_block(rng, own, number, rows, amount, top, most, lean):
    ranking = jax.random.permutation(rng, amount)
    crowded, ordinary = portions_of(amount, rows * top, most, lean, True), portions_of(amount, rows * top, most, lean, False)
    places = jnp.arange(amount)

    def named(sizes, turn):
        used = int((sizes > 0).sum())
        fixed = max(1, used // 4)
        moved = fixed + (places - fixed + turn * (used - fixed)) % max(1, amount - fixed)
        return jnp.zeros((amount,), jnp.int32).at[ranking[jnp.where(places < fixed, places, moved)]].set(jnp.asarray(sizes, jnp.int32))

    sizes = jnp.where(number % 4 == 0, named(crowded, number // 4), named(ordinary, number - number // 4 - 1))
    mixed = jax.random.permutation(jax.random.fold_in(own, 3), amount)
    giver, taker = mixed[0:amount // 2 * 2:2], mixed[1:amount // 2 * 2:2]
    margin = jnp.minimum(sizes[giver] - 1, most - sizes[taker]) // 2
    margin = jnp.where((giver == ranking[0]) | (taker == ranking[0]) | (sizes[taker] == 0), 0, jnp.maximum(margin, 0))
    moved = jax.random.randint(jax.random.fold_in(own, 4), (amount // 2,), 0, 1 << 20) % (margin + 1)
    sizes = sizes.at[giver].add(-moved).at[taker].add(moved)
    members = jnp.searchsorted(jnp.cumsum(sizes), jnp.arange(rows * top), side="right").astype(jnp.int32)
    grid = members.reshape(top, rows).T
    grid = grid[jax.random.permutation(jax.random.fold_in(own, 1), rows)]
    turn = jax.random.randint(jax.random.fold_in(own, 2), (rows, 1), 0, top)
    return jnp.take_along_axis(grid, (jnp.arange(top)[None, :] + turn) % top, axis=1)


def portions_of(number_of, total, reach, lean, full):
    portions = [(1 << 20) // math.isqrt(rank ** lean) + 1 for rank in range(1, number_of + 1)]
    largest = reach if full else min(reach, max(-(-total // number_of), total * portions[0] // sum(portions)))
    least = 1 if total - largest >= number_of - 1 else 0
    counts, rest = [largest] + [least] * (number_of - 1), total - largest - least * (number_of - 1)
    while rest > 0:
        movable = [i for i in range(1, number_of) if counts[i] < largest] or [i for i in range(1, number_of) if counts[i] < reach]
        pool, budget = sum([portions[i] for i in movable]), rest
        for i in movable:
            more = min(reach - counts[i], max(1, budget * portions[i] // pool), rest)
            counts[i] = counts[i] + more
            rest = rest - more
    return np.array(counts)


def scatter_about(stream_key, shape, spread, bound, pieces=(), kind=jnp.bfloat16):
    values = jax.random.normal(stream_key, shape, jnp.float32) * spread
    if len(pieces) > 0:
        values = levels(stream_key, shape, pieces, -0.22, 0.18) * values
    return jnp.clip(values, min=-bound, max=bound).astype(kind)


def setup_inputs(seed: int = 0, part: int = 0) -> dict:
    splits = jax.random.split(jax.random.key(seed), 6)
    part_keys = jax.random.split(jax.random.fold_in(splits[5], part), 6)
    expert_ids_keys = jax.random.split(jax.random.fold_in(part_keys[0], 1), TOKENS // TOK_DEV)
    expert_ids_turns = jax.random.permutation(jax.random.fold_in(part_keys[0], 3), TOKENS // TOK_DEV)
    expert_ids = jax.vmap(lambda own, number: routed_block(jax.random.fold_in(part_keys[0], 2), own, number, TOK_DEV, EXPERTS, TOP, CAP, 2))(expert_ids_keys, expert_ids_turns).reshape((TOKENS, TOP))
    route_gates = jnp.clip(0.1 + 0.4 * jax.random.uniform(part_keys[1], (TOKENS, TOP), jnp.float32) ** levels(part_keys[1], (TOKENS, TOP), ((0, 16),), -0.2, 0.2), 0.1, 0.5)
    routed_in = scatter_about(part_keys[2], (TOKENS, TOP, 2 * F), 1.0, 6.0, ((0, 16),))
    down_weight = scatter_about(splits[3], (EXPERTS, F, D), F ** -0.5, 0.1875, ((0, 16),))
    slot_offset = jax.random.randint(splits[4], (1,), 0, EXPERTS).astype(jnp.int32)
    return dict(expert_ids=expert_ids, route_gates=route_gates, routed_in=routed_in, down_weight=down_weight, slot_offset=slot_offset)


def swiglu(packed):
    half = packed.shape[-1] // 2
    gate = packed[..., :half].astype(jnp.float32)
    upper = packed[..., half:].astype(jnp.float32)
    return (jax.nn.silu(gate) * upper).astype(jnp.bfloat16)


def reference(expert_ids, route_gates, routed_in, down_weight, slot_offset):
    pairs = expert_ids.reshape(-1).astype(jnp.int32)
    pair_count = pairs.shape[0]
    most_rows = EXPERTS * CAP
    hidden = swiglu(routed_in).reshape(pair_count, F)
    order = jnp.argsort(pairs, stable=True).astype(jnp.int32)
    inverse = jnp.argsort(order, stable=True).astype(jnp.int32)
    sorted_hidden = jnp.concatenate([hidden[order], jnp.zeros((most_rows, F), jnp.bfloat16)], axis=0)
    loads = jnp.sum((pairs[:, None] == jnp.arange(EXPERTS, dtype=jnp.int32)[None, :]).astype(jnp.int32), axis=0)
    starts = (jnp.cumsum(loads) - loads).astype(jnp.int32)

    def one_expert(carry, expert):
        start = starts[expert]
        rows = lax.dynamic_slice_in_dim(sorted_hidden, start, most_rows, 0)
        matrix = down_weight[jnp.mod(expert - slot_offset[0], EXPERTS).astype(jnp.int32)]
        result = jnp.dot(rows, matrix, preferred_element_type=jnp.float32).astype(jnp.bfloat16)
        live = jnp.arange(most_rows, dtype=jnp.int32) < loads[expert]
        before = lax.dynamic_slice_in_dim(carry, start, most_rows, 0)
        update = jnp.where(live[:, None], result, before)
        return lax.dynamic_update_slice_in_dim(carry, update, start, 0), None

    initial = jnp.zeros((pair_count + most_rows, D), jnp.bfloat16)
    filled, unused = lax.scan(one_expert, initial, jnp.arange(EXPERTS, dtype=jnp.int32))
    outputs = filled[:pair_count][inverse].reshape(TOKENS, TOP, D)
    total = jnp.zeros((TOKENS, D), jnp.float32)
    for choice_index in range(TOP):
        total = total + route_gates[:, choice_index, None] * outputs[:, choice_index].astype(jnp.float32)
    return total.astype(jnp.bfloat16)
```

```python
import functools

import jax
import jax.numpy as jnp
from jax import lax
from jax.experimental import pallas as pl
from jax.experimental.pallas import tpu as pltpu
from jax.sharding import PartitionSpec as P

MESH = pl.DeviceIdType.MESH
TILE = 256
HALVES = 2
VMEM_LIMIT = 63 * 1024 * 1024


def swiglu(packed):
    half = packed.shape[-1] // 2
    gate = packed[..., :half].astype(jnp.float32)
    upper = packed[..., half:].astype(jnp.float32)
    return (jax.nn.silu(gate) * upper).astype(jnp.bfloat16)


def exchange_form(expert_ids, route_gates, routed_in, down_weight, slot_offset):
    experts = lax.axis_size("ep")
    tokens_here, chosen = expert_ids.shape
    pair_count = tokens_here * chosen
    capacity = 2 * pair_count // experts
    matrix = down_weight[0]
    offset = slot_offset[0]
    target = jnp.mod(expert_ids.reshape(pair_count) - offset, experts)
    onehot = (target[:, None] == jnp.arange(experts, dtype=jnp.int32)[None, :]).astype(jnp.int32)
    earlier = jnp.cumsum(onehot, axis=0) - onehot
    rank = jnp.sum(earlier * onehot, axis=1)
    row_index = target * capacity + rank
    source = (
        jnp.full((experts * capacity,), pair_count, jnp.int32)
        .at[row_index]
        .set(jnp.arange(pair_count, dtype=jnp.int32))
    )
    payload = swiglu(routed_in.reshape(pair_count, routed_in.shape[2]))
    padded = jnp.concatenate([payload, jnp.zeros((1, payload.shape[1]), jnp.bfloat16)], axis=0)
    outgoing = jnp.take(padded, source, axis=0).reshape(experts, capacity, payload.shape[1])
    results = jnp.einsum(
        "nkf,fd->nkd",
        lax.all_to_all(outgoing, "ep", split_axis=0, concat_axis=0, tiled=True),
        matrix,
        preferred_element_type=jnp.float32,
    ).astype(jnp.bfloat16)
    returned = lax.all_to_all(results, "ep", split_axis=0, concat_axis=0, tiled=True)
    width = returned.shape[2]
    picked = jnp.take(returned.reshape(experts * capacity, width), row_index, axis=0).reshape(
        tokens_here, chosen, width
    )
    total = jnp.zeros((tokens_here, width), jnp.float32)
    for choice_index in range(chosen):
        total = total + route_gates[:, choice_index, None] * picked[:, choice_index].astype(
            jnp.float32
        )
    return total.astype(jnp.bfloat16)


def flipped(index, distance):
    result, bit = index, 1
    while bit <= distance:
        if distance & bit:
            result = result + bit - 2 * bit * lax.rem(lax.div(index, bit), 2)
        bit *= 2
    return result


def slot_distance(group, slot):
    return group * 4 + (slot % 2) * 2 + slot // 2


def kernel(
    n,
    target_ref,
    gate_ref,
    x_hbm,
    w_hbm,
    out_ref,
    x,
    w,
    hid,
    outg,
    recv,
    own,
    psend,
    crecv,
    ysend,
    yrecv,
    zsend,
    zrecv,
    lsem,
    dsend_sem,
    drecv_sem,
    csend_sem,
    crecv_sem,
    ysend_sem,
    yrecv_sem,
    zsend_sem,
    zrecv_sem,
):
    me = lax.axis_index("ep")
    tokens, chosen = target_ref.shape
    pairs = tokens * chosen
    features = hid.shape[1]
    groups, halves, _, wide = own.shape

    barrier = pltpu.get_barrier_semaphore()
    for d in range(1, n):
        pl.semaphore_signal(barrier, inc=1, device_id={"ep": flipped(me, d)}, device_id_type=MESH)
    x_copy = pltpu.make_async_copy(x_hbm, x, lsem.at[0])
    x_copy.start()
    w_copy = pltpu.make_async_copy(w_hbm.at[0], w, lsem.at[1])
    w_copy.start()
    x_copy.wait()

    @pl.loop(0, tokens // 8)
    def _(block):
        rows = x[pl.ds(pl.multiple_of(block * 8, 8), 8)].astype(jnp.float32)
        rows = rows.reshape(8 * chosen, 2 * features)
        value = jax.nn.silu(rows[:, :features]) * rows[:, features:]
        start = pl.multiple_of(block * 8 * chosen, 8 * chosen)
        hid[pl.ds(start, 8 * chosen)] = value.astype(jnp.bfloat16)

    pl.semaphore_wait(barrier, n - 1)

    target = target_ref[...]
    gates = gate_ref[...]
    lane = lax.broadcasted_iota(jnp.int32, (chosen, pairs), 1)
    spread = (lane % chosen == lax.broadcasted_iota(jnp.int32, (chosen, pairs), 0)).astype(jnp.bfloat16)
    mine = (
        lax.broadcasted_iota(jnp.int32, (tokens, pairs), 1) // chosen
        == lax.broadcasted_iota(jnp.int32, (tokens, pairs), 0)
    )
    order = list(range(groups - 1, -1, -1))
    dispatch = {}
    for g in order:
        picks, scales = [], []
        for q in range(4):
            hit = target == flipped(me, slot_distance(g, q))
            scales.append(jnp.sum(jnp.where(hit, gates, 0.0), axis=1, keepdims=True))
            chosen_here = jnp.dot(
                hit.astype(jnp.float32).astype(jnp.bfloat16), spread, preferred_element_type=jnp.float32
            )
            picks.append(jnp.where(mine, chosen_here, 0.0).astype(jnp.bfloat16))
        pick = jnp.concatenate(picks, axis=0)
        scale = jnp.concatenate(scales, axis=0)
        for c in range(0, features, TILE):
            rows = jnp.dot(pick, hid[:, c : c + TILE], preferred_element_type=jnp.float32)
            rows = (rows * scale).astype(jnp.bfloat16)
            if g == 0:
                recv[0, 0:tokens, c : c + TILE] = rows[0:tokens]
                outg[0, tokens:, c : c + TILE] = rows[tokens:]
            else:
                outg[g, :, c : c + TILE] = rows
        for q in range(4):
            d = slot_distance(g, q)
            if d == 0:
                continue
            dispatch[d] = pltpu.make_async_remote_copy(
                src_ref=outg.at[g, pl.ds(q * tokens, tokens)],
                dst_ref=recv.at[g, pl.ds(q * tokens, tokens)],
                send_sem=dsend_sem.at[d],
                recv_sem=drecv_sem.at[d],
                device_id={"ep": flipped(me, d)},
                device_id_type=MESH,
            )
            dispatch[d].start()
    w_copy.wait()

    core, side, far = {}, {}, {}

    def finish_core(g, h):
        core[g, h].wait_recv()
        own[g, h, 0:tokens] = own[g, h, 0:tokens] + crecv[g, h, 0:tokens].astype(jnp.float32)
        ysend[g, h] = (own[g, h, tokens:] + crecv[g, h, tokens:].astype(jnp.float32)).astype(jnp.bfloat16)
        side[g, h] = pltpu.make_async_remote_copy(
            src_ref=ysend.at[g, h],
            dst_ref=yrecv.at[g, h],
            send_sem=ysend_sem.at[g, h],
            recv_sem=yrecv_sem.at[g, h],
            device_id={"ep": flipped(me, 2)},
            device_id_type=MESH,
        )
        side[g, h].start()

    def finish_side(g, h):
        side[g, h].wait_recv()
        value = own[g, h, 0:tokens] + yrecv[g, h].astype(jnp.float32)
        if g == 0:
            own[g, h, 0:tokens] = value
            return
        zsend[g - 1, h] = value.astype(jnp.bfloat16)
        far[g, h] = pltpu.make_async_remote_copy(
            src_ref=zsend.at[g - 1, h],
            dst_ref=zrecv.at[g - 1, h],
            send_sem=zsend_sem.at[g - 1, h],
            recv_sem=zrecv_sem.at[g - 1, h],
            device_id={"ep": flipped(me, 4 * g)},
            device_id_type=MESH,
        )
        far[g, h].start()

    for place, g in enumerate(order):
        for q in range(4):
            if slot_distance(g, q):
                dispatch[slot_distance(g, q)].wait_recv()
        for h in range(halves):

            @pl.loop(0, wide // TILE)
            def _(j):
                here = pl.ds(pl.multiple_of(j * TILE, TILE), TILE)
                there = pl.ds(pl.multiple_of(h * wide + j * TILE, TILE), TILE)
                result = jnp.dot(recv[g], w[:, there], preferred_element_type=jnp.float32)
                own[g, h, :, here] = result[: 2 * tokens]
                psend[g, h, :, here] = result[2 * tokens :].astype(jnp.bfloat16)

            core[g, h] = pltpu.make_async_remote_copy(
                src_ref=psend.at[g, h],
                dst_ref=crecv.at[g, h],
                send_sem=csend_sem.at[g, h],
                recv_sem=crecv_sem.at[g, h],
                device_id={"ep": flipped(me, 1)},
                device_id_type=MESH,
            )
            core[g, h].start()
        for h in range(halves):
            finish_core(g, h)
        if place:
            for h in range(halves):
                finish_side(order[place - 1], h)
    for h in range(halves):
        finish_side(0, h)
    for h in range(halves):
        total = own[0, h, 0:tokens]
        for g in order[:-1]:
            far[g, h].wait_recv()
            total = total + zrecv[g - 1, h].astype(jnp.float32)
        out_ref[:, h * wide : (h + 1) * wide] = total.astype(jnp.bfloat16)
    for copies in (dispatch, core, side, far):
        for copy in copies.values():
            copy.wait_send()


def scratch_of(n, tokens, chosen, features, width):
    groups, wide = n // 4, width // HALVES
    small = jnp.bfloat16
    return [
        ((tokens, chosen, 2 * features), small),
        ((features, width), small),
        ((tokens * chosen, features), small),
        ((groups, 4 * tokens, features), small),
        ((groups, 4 * tokens, features), small),
        ((groups, HALVES, 2 * tokens, wide), jnp.float32),
        ((groups, HALVES, 2 * tokens, wide), small),
        ((groups, HALVES, 2 * tokens, wide), small),
        ((groups, HALVES, tokens, wide), small),
        ((groups, HALVES, tokens, wide), small),
        ((max(groups - 1, 1), HALVES, tokens, wide), small),
        ((max(groups - 1, 1), HALVES, tokens, wide), small),
    ]


def bytes_of(buffers):
    total = 0
    for shape, kind in buffers:
        size = jnp.dtype(kind).itemsize
        for extent in shape:
            size *= extent
        total += size
    return total


def on_device(expert_ids, route_gates, routed_in, down_weight, slot_offset):
    n = lax.axis_size("ep")
    tokens, chosen = expert_ids.shape
    features, width = down_weight.shape[1:]
    buffers = scratch_of(n, tokens, chosen, features, width)
    if (
        n < 4
        or n & (n - 1)
        or tokens % 16
        or chosen % 8
        or features % TILE
        or width % (HALVES * TILE)
        or bytes_of(buffers) > VMEM_LIMIT * 3 // 4
    ):
        return exchange_form(expert_ids, route_gates, routed_in, down_weight, slot_offset)
    groups = n // 4
    target = jnp.mod(expert_ids - slot_offset[0], n)
    dma = pltpu.SemaphoreType.DMA
    pair = (groups, HALVES)
    far = (max(groups - 1, 1), HALVES)
    return pl.pallas_call(
        functools.partial(kernel, n),
        out_shape=jax.ShapeDtypeStruct((tokens, width), jnp.bfloat16),
        in_specs=[pl.BlockSpec(memory_space=pltpu.VMEM)] * 2 + [pl.BlockSpec(memory_space=pl.ANY)] * 2,
        out_specs=pl.BlockSpec(memory_space=pltpu.VMEM),
        scratch_shapes=[pltpu.VMEM(shape, kind) for shape, kind in buffers]
        + [dma((2,)), dma((n,)), dma((n,))]
        + [dma(pair)] * 4
        + [dma(far)] * 2,
        compiler_params=pltpu.CompilerParams(
            collective_id=0, has_side_effects=True, vmem_limit_bytes=VMEM_LIMIT
        ),
    )(target, route_gates, routed_in, down_weight)


def solution(mesh):
    placed = (
        P(("grp", "ep"), None),
        P(("grp", "ep"), None),
        P(("grp", "ep"), None, None),
        P("ep", None, None),
        P(),
    )
    return jax.shard_map(
        on_device, mesh=mesh, in_specs=placed, out_specs=P(("grp", "ep"), None), check_vma=False
    )
```

```python
import functools

import jax
import jax.numpy as jnp
from jax import lax
from jax.experimental import pallas as pl
from jax.experimental.pallas import tpu as pltpu
from jax.sharding import PartitionSpec as P

MESH = pl.DeviceIdType.MESH
TILE = 256
CHUNKS = 4
VMEM_LIMIT = 63 * 1024 * 1024


def swiglu(packed):
    half = packed.shape[-1] // 2
    gate = packed[..., :half].astype(jnp.float32)
    upper = packed[..., half:].astype(jnp.float32)
    return (jax.nn.silu(gate) * upper).astype(jnp.bfloat16)


def exchange_form(expert_ids, route_gates, routed_in, down_weight, slot_offset):
    experts = lax.axis_size("ep")
    tokens_here, chosen = expert_ids.shape
    pair_count = tokens_here * chosen
    capacity = 2 * pair_count // experts
    matrix = down_weight[0]
    offset = slot_offset[0]
    target = jnp.mod(expert_ids.reshape(pair_count) - offset, experts)
    onehot = (target[:, None] == jnp.arange(experts, dtype=jnp.int32)[None, :]).astype(jnp.int32)
    earlier = jnp.cumsum(onehot, axis=0) - onehot
    rank = jnp.sum(earlier * onehot, axis=1)
    row_index = target * capacity + rank
    source = (
        jnp.full((experts * capacity,), pair_count, jnp.int32)
        .at[row_index]
        .set(jnp.arange(pair_count, dtype=jnp.int32))
    )
    payload = swiglu(routed_in.reshape(pair_count, routed_in.shape[2]))
    padded = jnp.concatenate([payload, jnp.zeros((1, payload.shape[1]), jnp.bfloat16)], axis=0)
    outgoing = jnp.take(padded, source, axis=0).reshape(experts, capacity, payload.shape[1])
    results = jnp.einsum(
        "nkf,fd->nkd",
        lax.all_to_all(outgoing, "ep", split_axis=0, concat_axis=0, tiled=True),
        matrix,
        preferred_element_type=jnp.float32,
    ).astype(jnp.bfloat16)
    returned = lax.all_to_all(results, "ep", split_axis=0, concat_axis=0, tiled=True)
    width = returned.shape[2]
    picked = jnp.take(returned.reshape(experts * capacity, width), row_index, axis=0).reshape(
        tokens_here, chosen, width
    )
    total = jnp.zeros((tokens_here, width), jnp.float32)
    for choice_index in range(chosen):
        total = total + route_gates[:, choice_index, None] * picked[:, choice_index].astype(
            jnp.float32
        )
    return total.astype(jnp.bfloat16)


def flipped(index, distance):
    result, bit = index, 1
    while bit <= distance:
        if distance & bit:
            result = result + bit - 2 * bit * lax.rem(lax.div(index, bit), 2)
        bit *= 2
    return result


def slot_distance(n, slot):
    groups = n // 4
    return (groups - 1 - slot % groups) * 4 + (slot // groups % 2) * 2 + slot // (2 * groups)


def kernel(
    n,
    target_ref,
    gate_ref,
    x_hbm,
    w_hbm,
    out_ref,
    x,
    w,
    outg,
    recv,
    own,
    psend,
    crecv,
    ysend,
    yrecv,
    zsend,
    zrecv,
    wsem,
    xsem,
    dsend_sem,
    drecv_sem,
    csend_sem,
    crecv_sem,
    ysend_sem,
    yrecv_sem,
    zsend_sem,
    zrecv_sem,
):
    me = lax.axis_index("ep")
    chosen = target_ref.shape[1]
    features, width = w.shape
    chunks, rows_all, _ = recv.shape
    part = rows_all // n
    pairs = part * chosen
    groups = n // 4
    plane = groups * part

    def send(src, dst, send_sem, recv_sem, distance):
        copy = pltpu.make_async_remote_copy(
            src_ref=src,
            dst_ref=dst,
            send_sem=send_sem,
            recv_sem=recv_sem,
            device_id={"ep": flipped(me, distance)},
            device_id_type=MESH,
        )
        copy.start()
        return copy

    barrier = pltpu.get_barrier_semaphore()
    for d in range(1, n):
        pl.semaphore_signal(barrier, inc=1, device_id={"ep": flipped(me, d)}, device_id_type=MESH)
    x_copies = []
    for k in range(chunks):
        tokens_of = pl.ds(k * part, part)
        x_copies.append(pltpu.make_async_copy(x_hbm.at[tokens_of], x.at[tokens_of], xsem.at[k]))
        x_copies[k].start()
    w_copy = pltpu.make_async_copy(w_hbm.at[0], w, wsem.at[0])
    w_copy.start()

    lane = lax.broadcasted_iota(jnp.int32, (chosen, pairs), 1)
    spread = (lane % chosen == lax.broadcasted_iota(jnp.int32, (chosen, pairs), 0)).astype(jnp.bfloat16)
    mine = (
        lax.broadcasted_iota(jnp.int32, (rows_all, pairs), 1) // chosen
        == lax.broadcasted_iota(jnp.int32, (rows_all, pairs), 0) % part
    )
    slots = [slot_distance(n, s) for s in range(n)]
    peers = [flipped(me, d) for d in slots]
    dispatch = {}
    for k in range(chunks):
        target = target_ref[k * part : (k + 1) * part]
        gates = gate_ref[k * part : (k + 1) * part]
        hit = jnp.concatenate([jnp.where(target == e, 1.0, 0.0) for e in peers], axis=0)
        scale = jnp.sum(hit * jnp.concatenate([gates] * n, axis=0), axis=1, keepdims=True)
        wanted = jnp.dot(hit.astype(jnp.bfloat16), spread, preferred_element_type=jnp.float32)
        pick = jnp.where(mine, wanted, 0.0).astype(jnp.bfloat16)
        x_copies[k].wait()
        for c in range(0, features, TILE):
            gate = x[k * part : (k + 1) * part, :, c : c + TILE].astype(jnp.float32)
            upper = x[k * part : (k + 1) * part, :, features + c : features + c + TILE].astype(jnp.float32)
            hidden = (jax.nn.silu(gate) * upper).reshape(pairs, TILE).astype(jnp.bfloat16)
            rows = jnp.dot(pick, hidden, preferred_element_type=jnp.float32)
            rows = (rows * scale).astype(jnp.bfloat16)
            for s, d in enumerate(slots):
                if d:
                    outg[k, s * part : (s + 1) * part, c : c + TILE] = rows[s * part : (s + 1) * part]
                else:
                    recv[k, s * part : (s + 1) * part, c : c + TILE] = rows[s * part : (s + 1) * part]
        if k == 0:
            pl.semaphore_wait(barrier, n - 1)
        for d in range(n - 1, 0, -1):
            s = slots.index(d)
            here = pl.ds(s * part, part)
            dispatch[k, s] = send(
                outg.at[k, here], recv.at[k, here], dsend_sem.at[k, s], drecv_sem.at[k, s], d
            )
    w_copy.wait()

    core, side, line = {}, {}, {}

    def row_of(dz):
        return pl.ds((groups - 1 - dz) * part, part)

    def multiply(k):
        for s, d in enumerate(slots):
            if d:
                dispatch[k, s].wait_recv()

        @pl.loop(0, width // TILE)
        def _(j):
            here = pl.ds(pl.multiple_of(j * TILE, TILE), TILE)
            result = jnp.dot(recv[k], w[:, here], preferred_element_type=jnp.float32)
            own[k, :, here] = result[: 2 * plane]
            psend[k, :, here] = result[2 * plane :].astype(jnp.bfloat16)

        core[k] = send(psend.at[k], crecv.at[k], csend_sem.at[k], crecv_sem.at[k], 1)

    def finish_core(k):
        core[k].wait_recv()
        for p in range(2):
            here = pl.ds(p * plane // 2, plane // 2)
            there = pl.ds(plane + p * plane // 2, plane // 2)
            ysend[k, here] = (own[k, there] + crecv[k, there].astype(jnp.float32)).astype(jnp.bfloat16)
            side[k, p] = send(
                ysend.at[k, here], yrecv.at[k, here], ysend_sem.at[k, p], yrecv_sem.at[k, p], 2
            )
        own[k, 0:plane] = own[k, 0:plane] + crecv[k, 0:plane].astype(jnp.float32)

    def start_line(k, dz, bit, value):
        zsend[k, dz] = value.astype(jnp.bfloat16)
        line[k, dz] = send(
            zsend.at[k, dz], zrecv.at[k, dz], zsend_sem.at[k, dz], zrecv_sem.at[k, dz], 4 * bit
        )

    def finish_side(k):
        for p in range(2):
            side[k, p].wait_recv()
            for dz in range(groups - 1 - p * groups // 2, groups // 2 - 1 - p * groups // 2, -1):
                value = own[k, row_of(dz)] + yrecv[k, row_of(dz)].astype(jnp.float32)
                if dz % 2:
                    start_line(k, dz, 1, value)
                else:
                    own[k, row_of(dz)] = value

    def finish_line(k, bit):
        for dz in range(groups - 2 * bit, -1, -2 * bit):
            line[k, dz + bit].wait_recv()
            value = own[k, row_of(dz)] + zrecv[k, dz + bit].astype(jnp.float32)
            if dz == 0 and 2 * bit == groups:
                out_ref[k * part : (k + 1) * part] = value.astype(jnp.bfloat16)
            elif dz % (4 * bit):
                start_line(k, dz, 2 * bit, value)
            else:
                own[k, row_of(dz)] = value

    levels = groups.bit_length() - 1
    for turn in range(chunks + 1 + levels):
        if turn < chunks:
            multiply(turn)
            finish_core(turn)
        for level in range(levels - 1, -1, -1):
            if 0 <= turn - 2 - level < chunks:
                finish_line(turn - 2 - level, 1 << level)
        if 0 <= turn - 1 < chunks:
            finish_side(turn - 1)
    for copies in (dispatch, core, side, line):
        for copy in copies.values():
            copy.wait_send()


def scratch_of(n, tokens, chosen, features, width):
    part = tokens // CHUNKS
    plane = n // 4 * part
    small = jnp.bfloat16
    return [
        ((tokens, chosen, 2 * features), small),
        ((features, width), small),
        ((CHUNKS, n * part, features), small),
        ((CHUNKS, n * part, features), small),
        ((CHUNKS, 2 * plane, width), jnp.float32),
        ((CHUNKS, 2 * plane, width), small),
        ((CHUNKS, 2 * plane, width), small),
        ((CHUNKS, plane, width), small),
        ((CHUNKS, plane, width), small),
        ((CHUNKS, n // 4, part, width), small),
        ((CHUNKS, n // 4, part, width), small),
    ]


def bytes_of(buffers):
    total = 0
    for shape, kind in buffers:
        size = jnp.dtype(kind).itemsize
        for extent in shape:
            size *= extent
        total += size
    return total


def on_device(expert_ids, route_gates, routed_in, down_weight, slot_offset):
    n = lax.axis_size("ep")
    tokens, chosen = expert_ids.shape
    features, width = down_weight.shape[1:]
    buffers = scratch_of(n, tokens, chosen, features, width)
    if (
        n < 8
        or n & (n - 1)
        or tokens % (16 * CHUNKS)
        or chosen % 8
        or features % TILE
        or width % TILE
        or bytes_of(buffers) > VMEM_LIMIT * 3 // 4
    ):
        return exchange_form(expert_ids, route_gates, routed_in, down_weight, slot_offset)
    target = jnp.mod(expert_ids - slot_offset[0], n)
    dma = pltpu.SemaphoreType.DMA
    return pl.pallas_call(
        functools.partial(kernel, n),
        out_shape=jax.ShapeDtypeStruct((tokens, width), jnp.bfloat16),
        in_specs=[pl.BlockSpec(memory_space=pltpu.VMEM)] * 2 + [pl.BlockSpec(memory_space=pl.ANY)] * 2,
        out_specs=pl.BlockSpec(memory_space=pltpu.VMEM),
        scratch_shapes=[pltpu.VMEM(shape, kind) for shape, kind in buffers]
        + [dma((1,)), dma((CHUNKS,))]
        + [dma((CHUNKS, n))] * 2
        + [dma((CHUNKS,))] * 2
        + [dma((CHUNKS, 2))] * 2
        + [dma((CHUNKS, n // 4))] * 2,
        compiler_params=pltpu.CompilerParams(
            collective_id=0, has_side_effects=True, vmem_limit_bytes=VMEM_LIMIT
        ),
    )(target, route_gates, routed_in, down_weight)


def solution(mesh):
    placed = (
        P(("grp", "ep"), None),
        P(("grp", "ep"), None),
        P(("grp", "ep"), None, None),
        P("ep", None, None),
        P(),
    )
    return jax.shard_map(
        on_device, mesh=mesh, in_specs=placed, out_specs=P(("grp", "ep"), None), check_vma=False
    )
```

```python
import functools

import jax
import jax.numpy as jnp
from jax import lax
from jax.experimental import pallas as pl
from jax.experimental.pallas import tpu as pltpu
from jax.sharding import PartitionSpec as P

MESH = pl.DeviceIdType.MESH
TILE = 256
CHUNKS = 4
AHEAD = 3
VMEM_LIMIT = 63 * 1024 * 1024


def swiglu(packed):
    half = packed.shape[-1] // 2
    gate = packed[..., :half].astype(jnp.float32)
    upper = packed[..., half:].astype(jnp.float32)
    return (jax.nn.silu(gate) * upper).astype(jnp.bfloat16)


def exchange_form(expert_ids, route_gates, routed_in, down_weight, slot_offset):
    experts = lax.axis_size("ep")
    tokens_here, chosen = expert_ids.shape
    pair_count = tokens_here * chosen
    capacity = 2 * pair_count // experts
    matrix = down_weight[0]
    offset = slot_offset[0]
    target = jnp.mod(expert_ids.reshape(pair_count) - offset, experts)
    onehot = (target[:, None] == jnp.arange(experts, dtype=jnp.int32)[None, :]).astype(jnp.int32)
    earlier = jnp.cumsum(onehot, axis=0) - onehot
    rank = jnp.sum(earlier * onehot, axis=1)
    row_index = target * capacity + rank
    source = (
        jnp.full((experts * capacity,), pair_count, jnp.int32)
        .at[row_index]
        .set(jnp.arange(pair_count, dtype=jnp.int32))
    )
    payload = swiglu(routed_in.reshape(pair_count, routed_in.shape[2]))
    padded = jnp.concatenate([payload, jnp.zeros((1, payload.shape[1]), jnp.bfloat16)], axis=0)
    outgoing = jnp.take(padded, source, axis=0).reshape(experts, capacity, payload.shape[1])
    results = jnp.einsum(
        "nkf,fd->nkd",
        lax.all_to_all(outgoing, "ep", split_axis=0, concat_axis=0, tiled=True),
        matrix,
        preferred_element_type=jnp.float32,
    ).astype(jnp.bfloat16)
    returned = lax.all_to_all(results, "ep", split_axis=0, concat_axis=0, tiled=True)
    width = returned.shape[2]
    picked = jnp.take(returned.reshape(experts * capacity, width), row_index, axis=0).reshape(
        tokens_here, chosen, width
    )
    total = jnp.zeros((tokens_here, width), jnp.float32)
    for choice_index in range(chosen):
        total = total + route_gates[:, choice_index, None] * picked[:, choice_index].astype(
            jnp.float32
        )
    return total.astype(jnp.bfloat16)


def flipped(index, distance):
    result, bit = index, 1
    while bit <= distance:
        if distance & bit:
            result = result + bit - 2 * bit * lax.rem(lax.div(index, bit), 2)
        bit *= 2
    return result


def slot_distance(n, slot):
    groups = n // 4
    return (groups - 1 - slot % groups) * 4 + (slot // groups % 2) * 2 + slot // (2 * groups)


def kernel(
    n,
    target_ref,
    gate_ref,
    x_hbm,
    w_hbm,
    out_ref,
    x,
    w,
    outg,
    recv,
    own,
    psend,
    crecv,
    ysend,
    yrecv,
    zsend,
    zrecv,
    wsem,
    xsem,
    dsend_sem,
    drecv_sem,
    csend_sem,
    crecv_sem,
    ysend_sem,
    yrecv_sem,
    zsend_sem,
    zrecv_sem,
):
    me = lax.axis_index("ep")
    chosen = target_ref.shape[1]
    features, width = w.shape
    chunks, rows_all, _ = recv.shape
    part = rows_all // n
    pairs = part * chosen
    groups = n // 4
    plane = groups * part

    def send(src, dst, send_sem, recv_sem, distance):
        copy = pltpu.make_async_remote_copy(
            src_ref=src,
            dst_ref=dst,
            send_sem=send_sem,
            recv_sem=recv_sem,
            device_id={"ep": flipped(me, distance)},
            device_id_type=MESH,
        )
        copy.start()
        return copy

    barrier = pltpu.get_barrier_semaphore()
    for d in range(1, n):
        pl.semaphore_signal(barrier, inc=1, device_id={"ep": flipped(me, d)}, device_id_type=MESH)
    x_copies = []
    for k in range(chunks):
        tokens_of = pl.ds(k * part, part)
        x_copies.append(pltpu.make_async_copy(x_hbm.at[tokens_of], x.at[tokens_of], xsem.at[k]))
        x_copies[k].start()
    w_copy = pltpu.make_async_copy(w_hbm.at[0], w, wsem.at[0])
    w_copy.start()

    lane = lax.broadcasted_iota(jnp.int32, (chosen, pairs), 1)
    spread = (lane % chosen == lax.broadcasted_iota(jnp.int32, (chosen, pairs), 0)).astype(jnp.bfloat16)
    mine = (
        lax.broadcasted_iota(jnp.int32, (rows_all, pairs), 1) // chosen
        == lax.broadcasted_iota(jnp.int32, (rows_all, pairs), 0) % part
    )
    slots = [slot_distance(n, s) for s in range(n)]
    peers = [flipped(me, d) for d in slots]
    dispatch = {}

    def issue(k):
        for d in range(1, n):
            s = slots.index(d)
            here = pl.ds(s * part, part)
            dispatch[k, s] = send(
                outg.at[k, here], recv.at[k, here], dsend_sem.at[k, s], drecv_sem.at[k, s], d
            )

    for k in range(chunks):
        target = target_ref[k * part : (k + 1) * part]
        gates = gate_ref[k * part : (k + 1) * part]
        hit = jnp.concatenate([jnp.where(target == e, 1.0, 0.0) for e in peers], axis=0)
        scale = jnp.sum(hit * jnp.concatenate([gates] * n, axis=0), axis=1, keepdims=True)
        wanted = jnp.dot(hit.astype(jnp.bfloat16), spread, preferred_element_type=jnp.float32)
        pick = jnp.where(mine, wanted, 0.0).astype(jnp.bfloat16)
        x_copies[k].wait()
        for c in range(0, features, TILE):
            gate = x[k * part : (k + 1) * part, :, c : c + TILE].astype(jnp.float32)
            upper = x[k * part : (k + 1) * part, :, features + c : features + c + TILE].astype(jnp.float32)
            hidden = (jax.nn.silu(gate) * upper).reshape(pairs, TILE).astype(jnp.bfloat16)
            rows = jnp.dot(pick, hidden, preferred_element_type=jnp.float32)
            rows = (rows * scale).astype(jnp.bfloat16)
            for s, d in enumerate(slots):
                if d:
                    outg[k, s * part : (s + 1) * part, c : c + TILE] = rows[s * part : (s + 1) * part]
                else:
                    recv[k, s * part : (s + 1) * part, c : c + TILE] = rows[s * part : (s + 1) * part]
        if k == 0:
            pl.semaphore_wait(barrier, n - 1)
        if k < AHEAD:
            issue(k)
    w_copy.wait()

    core, side, line = {}, {}, {}

    def row_of(dz):
        return pl.ds((groups - 1 - dz) * part, part)

    def multiply(k):
        for s, d in enumerate(slots):
            if d:
                dispatch[k, s].wait_recv()

        @pl.loop(0, width // TILE)
        def _(j):
            here = pl.ds(pl.multiple_of(j * TILE, TILE), TILE)
            result = jnp.dot(recv[k], w[:, here], preferred_element_type=jnp.float32)
            own[k, :, here] = result[: 2 * plane]
            psend[k, :, here] = result[2 * plane :].astype(jnp.bfloat16)

        core[k] = send(psend.at[k], crecv.at[k], csend_sem.at[k], crecv_sem.at[k], 1)

    def finish_core(k):
        core[k].wait_recv()
        for p in range(2):
            here = pl.ds(p * plane // 2, plane // 2)
            there = pl.ds(plane + p * plane // 2, plane // 2)
            ysend[k, here] = (own[k, there] + crecv[k, there].astype(jnp.float32)).astype(jnp.bfloat16)
            side[k, p] = send(
                ysend.at[k, here], yrecv.at[k, here], ysend_sem.at[k, p], yrecv_sem.at[k, p], 2
            )
        own[k, 0:plane] = own[k, 0:plane] + crecv[k, 0:plane].astype(jnp.float32)

    def start_line(k, dz, bit, value):
        zsend[k, dz] = value.astype(jnp.bfloat16)
        line[k, dz] = send(
            zsend.at[k, dz], zrecv.at[k, dz], zsend_sem.at[k, dz], zrecv_sem.at[k, dz], 4 * bit
        )

    def finish_side(k):
        for p in range(2):
            side[k, p].wait_recv()
            for dz in range(groups - 1 - p * groups // 2, groups // 2 - 1 - p * groups // 2, -1):
                value = own[k, row_of(dz)] + yrecv[k, row_of(dz)].astype(jnp.float32)
                if dz % 2:
                    start_line(k, dz, 1, value)
                else:
                    own[k, row_of(dz)] = value

    def finish_line(k, bit):
        for dz in range(groups - 2 * bit, -1, -2 * bit):
            line[k, dz + bit].wait_recv()
            value = own[k, row_of(dz)] + zrecv[k, dz + bit].astype(jnp.float32)
            if dz == 0 and 2 * bit == groups:
                out_ref[k * part : (k + 1) * part] = value.astype(jnp.bfloat16)
            elif dz % (4 * bit):
                start_line(k, dz, 2 * bit, value)
            else:
                own[k, row_of(dz)] = value

    levels = groups.bit_length() - 1
    for turn in range(chunks + 1 + levels):
        if turn < chunks:
            multiply(turn)
            finish_core(turn)
            if turn + AHEAD < chunks:
                issue(turn + AHEAD)
        for level in range(levels - 1, -1, -1):
            if 0 <= turn - 2 - level < chunks:
                finish_line(turn - 2 - level, 1 << level)
        if 0 <= turn - 1 < chunks:
            finish_side(turn - 1)
    for copies in (dispatch, core, side, line):
        for copy in copies.values():
            copy.wait_send()


def scratch_of(n, tokens, chosen, features, width):
    part = tokens // CHUNKS
    plane = n // 4 * part
    small = jnp.bfloat16
    return [
        ((tokens, chosen, 2 * features), small),
        ((features, width), small),
        ((CHUNKS, n * part, features), small),
        ((CHUNKS, n * part, features), small),
        ((CHUNKS, 2 * plane, width), jnp.float32),
        ((CHUNKS, 2 * plane, width), small),
        ((CHUNKS, 2 * plane, width), small),
        ((CHUNKS, plane, width), small),
        ((CHUNKS, plane, width), small),
        ((CHUNKS, n // 4, part, width), small),
        ((CHUNKS, n // 4, part, width), small),
    ]


def bytes_of(buffers):
    total = 0
    for shape, kind in buffers:
        size = jnp.dtype(kind).itemsize
        for extent in shape:
            size *= extent
        total += size
    return total


def on_device(expert_ids, route_gates, routed_in, down_weight, slot_offset):
    n = lax.axis_size("ep")
    tokens, chosen = expert_ids.shape
    features, width = down_weight.shape[1:]
    buffers = scratch_of(n, tokens, chosen, features, width)
    if (
        n < 8
        or n & (n - 1)
        or tokens % (16 * CHUNKS)
        or chosen % 8
        or features % TILE
        or width % TILE
        or bytes_of(buffers) > VMEM_LIMIT * 3 // 4
    ):
        return exchange_form(expert_ids, route_gates, routed_in, down_weight, slot_offset)
    target = jnp.mod(expert_ids - slot_offset[0], n)
    dma = pltpu.SemaphoreType.DMA
    return pl.pallas_call(
        functools.partial(kernel, n),
        out_shape=jax.ShapeDtypeStruct((tokens, width), jnp.bfloat16),
        in_specs=[pl.BlockSpec(memory_space=pltpu.VMEM)] * 2 + [pl.BlockSpec(memory_space=pl.ANY)] * 2,
        out_specs=pl.BlockSpec(memory_space=pltpu.VMEM),
        scratch_shapes=[pltpu.VMEM(shape, kind) for shape, kind in buffers]
        + [dma((1,)), dma((CHUNKS,))]
        + [dma((CHUNKS, n))] * 2
        + [dma((CHUNKS,))] * 2
        + [dma((CHUNKS, 2))] * 2
        + [dma((CHUNKS, n // 4))] * 2,
        compiler_params=pltpu.CompilerParams(
            collective_id=0, has_side_effects=True, vmem_limit_bytes=VMEM_LIMIT
        ),
    )(target, route_gates, routed_in, down_weight)


def solution(mesh):
    placed = (
        P(("grp", "ep"), None),
        P(("grp", "ep"), None),
        P(("grp", "ep"), None, None),
        P("ep", None, None),
        P(),
    )
    return jax.shard_map(
        on_device, mesh=mesh, in_specs=placed, out_specs=P(("grp", "ep"), None), check_vma=False
    )
```
